32 devices in a mesh: surf: 8 (over y, x, core), probe: 4 (over z).
Axes of the slice: x: 2, y: 2, z: 4, core: 2. Of those that a mesh axis runs over, the one named last changes fastest.
Arguments:
- probes: bfloat16 [32, 65536], P('probe', 'surf'), may hold values from -6 to 6
- sigma: float32 [65536], P('surf'), may hold values from 0.5 to 2
- prior_patch: bfloat16 [128, 128], replicated, may hold values from -0.5 to 0.5
- owner_map: int32 [1024], P('surf'), may hold values from 0 to 7, as said below
- block_perm: int32 [1024], P('surf'), may hold values from 0 to 127, as said below
- col_counts: int32 [1024], P('surf'), may hold values from 1 to 64
- coef: bfloat16 [1024, 1024], P('surf'), may hold values from 0.5 to 1.5
- obs_weight: bfloat16 [1024, 64], P('surf'), may hold values from 0.25 to 1
- column_op: bfloat16 [1024, 1024], replicated, may hold values from -0.1875 to 0.1875
Outputs:
- hess: float32 [32, 65536], P('probe', 'surf')
- diag_est: float32 [65536], P('surf')
- quad: float32 [32], P('probe')
The draws below stay inside these ranges and needn't reach their ends.
Inputs may be any that keep to these rules, and one draw needn't show every extreme that they name: `owner_map`: the 128 blocks of each surface device go to 8 different column owners, 16 to each. The pairs (owner_map, block_perm) name every slot of every column owner exactly once; a column owner receives 16 blocks from each of 8 surface devices.
All inputs are finite; a program needn't handle non-finite values.
Results may differ from the reference program's by a relative error of at most 0.005.
Values may be sent and summed in bfloat16 or wider, within the bound.
No kernel may reach another device: no remote copies, remote signals or barrier semaphores. Data moves between devices by JAX's collectives and lax.ppermute only.
A program may use at most 64 MiB of HBM per device.

```python
import math
import jax
import jax.numpy as jnp
from jax import lax

P_SIZE = 32
BS = 64
PATCH = 128
NBD = 128
CAP = 16
NB = 1024
NS = 65536
VOL = 1024
N_SURF = 8


def owner_and_slot(key):
    groups = NBD // CAP
    key_order = jax.random.fold_in(key, 11)
    key_offset = jax.random.fold_in(key, 12)
    key_blocks = jax.random.fold_in(key, 13)
    key_slots = jax.random.fold_in(key, 14)
    relabel = jax.random.permutation(key_order, N_SURF)
    place = jnp.argsort(relabel)
    offsets = jax.random.permutation(key_offset, N_SURF)[:groups]
    order = jax.vmap(lambda k: jax.random.permutation(k, NBD))(jax.random.split(key_blocks, N_SURF))
    position = jnp.argsort(order, axis=1)
    group = position // CAP
    within = position % CAP
    owner = relabel[(place[:, None] - offsets[group]) % N_SURF]
    slot_tables = jax.vmap(lambda k: jax.random.permutation(k, NBD))(jax.random.split(key_slots, N_SURF))
    slot = slot_tables[owner, group * CAP + within]
    return (owner.reshape(-1).astype(jnp.int32), slot.reshape(-1).astype(jnp.int32))


def draw_owner_map(key, part):
    return owner_and_slot(key)[0]


def draw_block_perm(key, part):
    return owner_and_slot(key)[1]


def place_ends(entries, own_key, low, largest):
    longest = entries.shape.index(max(entries.shape))
    spots = []
    for shift in (0, 1):
        where = [jax.random.randint(jax.random.fold_in(own_key, axis), (), 0, length) for axis, length in enumerate(entries.shape)]
        where[longest] = (where[longest] + shift) % entries.shape[longest]
        spots.append(tuple(where))
    return entries.at[spots[0]].set(low).at[spots[1]].set(largest)


def level_of(key, shape, pieces, least, high):
    def one(dim, parts):
        heights = jax.random.uniform(jax.random.fold_in(jax.random.fold_in(key, 6), dim), (parts,), jnp.float32, least / len(pieces), high / len(pieces))
        return jnp.repeat(jnp.exp(heights), shape[dim] // parts).reshape((-1,) + (1,) * (len(shape) - dim - 1))

    loudness = one(*pieces[0])
    for cut in pieces[1:]:
        loudness = loudness * one(*cut)
    return loudness


def noise(rng, extent, scale, most, cuts=(), kind=jnp.bfloat16):
    values = jax.random.normal(rng, extent, jnp.float32) * scale
    if len(cuts) > 0:
        values = level_of(rng, extent, cuts, -0.22, 0.18) * values
    return jnp.clip(values, min=-most, max=most).astype(kind)


def setup_inputs(seed: int = 0) -> dict:
    arg_keys = jax.random.split(jax.random.key(seed), 10)
    probes = noise(arg_keys[0], (P_SIZE, NS), 1.0, 6.0, ((0, 4), (1, 8)))
    sigma = jnp.clip(jnp.exp(math.log(2.0) - 1.3862944 * jax.random.uniform(arg_keys[1], (NS,), jnp.float32) ** level_of(arg_keys[1], (NS,), ((0, 8),), -0.2, 0.2)), 0.5, 2.0)
    prior_patch = noise(arg_keys[2], (PATCH, PATCH), PATCH ** -0.5, 0.5)
    owner_map = draw_owner_map(jax.random.fold_in(arg_keys[9], 71), 0)
    block_perm = draw_block_perm(jax.random.fold_in(arg_keys[9], 71), 0)
    col_counts = place_ends(jax.random.randint(arg_keys[5], (NB,), 1, BS + 1), jax.random.fold_in(arg_keys[5], 1), 1, BS).astype(jnp.int32)
    coef = jnp.clip(0.5 + 1.0 * jax.random.uniform(arg_keys[6], (NB, VOL), jnp.float32) ** level_of(arg_keys[6], (NB, VOL), ((0, 8),), -0.2, 0.2), 0.5, 1.5).astype(jnp.bfloat16)
    obs_weight = jnp.clip(0.25 + 0.75 * jax.random.uniform(arg_keys[7], (NB, BS), jnp.float32) ** level_of(arg_keys[7], (NB, BS), ((0, 8),), -0.2, 0.2), 0.25, 1.0).astype(jnp.bfloat16)
    column_op = noise(arg_keys[8], (VOL, VOL), VOL ** -0.5, 0.1875)
    return dict(probes=probes, sigma=sigma, prior_patch=prior_patch, owner_map=owner_map, block_perm=block_perm, col_counts=col_counts, coef=coef, obs_weight=obs_weight, column_op=column_op)


def column_term(fields, coef_rows, obs_rows, counts, valid, column_op):
    rows, width, cols = fields.shape
    layers = coef_rows.shape[1] // cols
    column = lax.broadcasted_iota(jnp.int32, (rows, cols), 1)
    keep = jnp.where((column < counts[:, None]) & valid[:, None], 1.0, 0.0).astype(jnp.float32)
    coef_full = coef_rows.astype(jnp.float32).reshape(rows, 1, layers, cols) * keep[:, None, None, :]
    lifted = (fields.astype(jnp.float32)[:, :, None, :] * coef_full).astype(jnp.bfloat16)
    state = jnp.dot(lifted.reshape(rows * width, layers * cols), column_op, preferred_element_type=jnp.float32)
    weighted = (state.reshape(rows, width, layers, cols) * obs_rows.astype(jnp.float32)[:, None, None, :]).astype(jnp.bfloat16)
    adjoint = lax.dot_general(weighted.reshape(rows * width, layers * cols), column_op, (((1,), (1,)), ((), ())), preferred_element_type=jnp.float32)
    return jnp.sum(adjoint.reshape(rows, width, layers, cols) * coef_full, axis=2)


def reference(probes, sigma, prior_patch, owner_map, block_perm, col_counts, coef, obs_weight, column_op):
    grouped = probes.reshape(P_SIZE, NS // PATCH, PATCH).astype(jnp.float32)
    mixed = jnp.einsum("pki,ij->pkj", grouped, prior_patch.astype(jnp.float32))
    spread = (mixed.reshape(P_SIZE, NS) * sigma[None, :]).astype(jnp.bfloat16)
    fields = spread.reshape(P_SIZE, NB, BS).transpose(1, 0, 2)
    target = (owner_map * NBD + block_perm).astype(jnp.int32)
    coef_rows = coef[target]
    obs_rows = obs_weight[target]
    valid = jnp.ones((NBD,), dtype=bool)

    def one_group(items):
        return column_term(items[0], items[1], items[2], items[3], valid, column_op)

    sens = lax.map(one_group, (fields.reshape(N_SURF, NBD, P_SIZE, BS), coef_rows.reshape(N_SURF, NBD, VOL), obs_rows.reshape(N_SURF, NBD, BS), col_counts.reshape(N_SURF, NBD)))
    sens = sens.reshape(NB, P_SIZE, BS).transpose(1, 0, 2).reshape(P_SIZE, NS)
    scaled = (sens * sigma[None, :]).reshape(P_SIZE, NS // PATCH, PATCH)
    back = jnp.einsum("pkj,ij->pki", scaled, prior_patch.astype(jnp.float32), precision=lax.Precision.HIGHEST).reshape(P_SIZE, NS)
    values = probes.astype(jnp.float32)
    hess = values + back
    product = values * back
    diag_est = jnp.sum(product, axis=0) / P_SIZE
    quad = jnp.sum(product, axis=1)
    return hess, diag_est, quad
```

```python
import jax
import jax.numpy as jnp
from jax import lax
from jax.sharding import PartitionSpec as P

P_SIZE = 32
BS = 64
PATCH = 128


def column_term(fields, coef_rows, obs_rows, counts, valid, column_op):
    rows, width, cols = fields.shape
    layers = coef_rows.shape[1] // cols
    column = lax.broadcasted_iota(jnp.int32, (rows, cols), 1)
    keep = jnp.where((column < counts[:, None]) & valid[:, None], 1.0, 0.0).astype(jnp.float32)
    coef_full = (
        coef_rows.astype(jnp.float32).reshape(rows, 1, layers, cols) * keep[:, None, None, :]
    )
    lifted = (fields.astype(jnp.float32)[:, :, None, :] * coef_full).astype(jnp.bfloat16)
    state = jnp.dot(
        lifted.reshape(rows * width, layers * cols), column_op, preferred_element_type=jnp.float32
    )
    weighted = (
        state.reshape(rows, width, layers, cols) * obs_rows.astype(jnp.float32)[:, None, None, :]
    ).astype(jnp.bfloat16)
    adjoint = lax.dot_general(
        weighted.reshape(rows * width, layers * cols),
        column_op,
        (((1,), (1,)), ((), ())),
        preferred_element_type=jnp.float32,
    )
    return jnp.sum(adjoint.reshape(rows, width, layers, cols) * coef_full, axis=2)


def total_over(part, axis):
    size = lax.axis_size(axis)
    total = part
    for shift in range(size - 1, 0, -1):
        total = total + lax.ppermute(part, axis, [(i, partner(i, shift, size)) for i in range(size)])
    return total


def partner(i, shift, size):
    return i ^ shift if size & (size - 1) == 0 else (i + shift) % size


def halving_sum(part, axis):
    size = lax.axis_size(axis)
    if size & (size - 1):
        return lax.psum(part, axis)
    step = 1
    while step < size:
        part = part + lax.ppermute(part, axis, [(i, i ^ step) for i in range(size)])
        step *= 2
    return part


def body(
    probes, sigma, prior_patch, owner_map, block_perm, col_counts, coef, obs_weight, column_op
):
    width, nodes = probes.shape
    blocks = owner_map.shape[0]
    peers = lax.axis_size("surf")
    depth = max(1, blocks // peers)
    slots_all = peers * depth
    grouped = probes.reshape(width, nodes // PATCH, PATCH)
    mixed = jnp.einsum("pki,ij->pkj", grouped, prior_patch, preferred_element_type=jnp.float32)
    spread = (mixed.reshape(width, nodes) * sigma[None, :]).astype(jnp.bfloat16)
    fields = spread.reshape(width, blocks, BS).transpose(1, 0, 2)
    row_ids = lax.broadcasted_iota(jnp.int32, (blocks, blocks), 0)
    col_ids = lax.broadcasted_iota(jnp.int32, (blocks, blocks), 1)
    same = (owner_map[None, :] == owner_map[:, None]) & (col_ids < row_ids)
    rank = jnp.sum(same.astype(jnp.int32), axis=1)
    position = owner_map * depth + rank
    request = (
        jnp.full((slots_all,), -1, jnp.int32).at[position].set(block_perm).reshape(peers, depth)
    )
    asked = lax.all_to_all(request, "surf", split_axis=0, concat_axis=0, tiled=True)
    wanted = asked >= 0
    safe_asked = jnp.maximum(asked, 0)
    coef_out = jnp.where(wanted[:, :, None], coef[safe_asked], jnp.zeros((), jnp.bfloat16))
    obs_out = jnp.where(wanted[:, :, None], obs_weight[safe_asked], jnp.zeros((), jnp.bfloat16))
    coef_in, obs_in = (
        lax.all_to_all(coef_out, "surf", split_axis=0, concat_axis=0, tiled=True),
        lax.all_to_all(obs_out, "surf", split_axis=0, concat_axis=0, tiled=True),
    )
    coef_rows = coef_in.reshape(slots_all, coef.shape[1])[position]
    obs_rows = obs_in.reshape(slots_all, BS)[position]
    everyone = jnp.ones((blocks,), dtype=bool)
    sens = column_term(fields, coef_rows, obs_rows, col_counts, everyone, column_op)
    sens = sens.transpose(1, 0, 2).reshape(width, nodes)
    scaled = (sens * sigma[None, :]).reshape(width, nodes // PATCH, PATCH)
    back = jnp.einsum(
        "pkj,ij->pki", scaled, prior_patch.astype(jnp.float32), precision=lax.Precision.HIGHEST
    ).reshape(width, nodes)
    values = probes.astype(jnp.float32)
    hess = values + back
    product = values * back
    diag_est = total_over(jnp.sum(product, axis=0), "probe") / P_SIZE
    quad = halving_sum(jnp.sum(product, axis=1), "surf")
    return (hess, diag_est, quad)


def solution(mesh):
    in_specs = (
        P("probe", "surf"),
        P("surf"),
        P(),
        P("surf"),
        P("surf"),
        P("surf"),
        P("surf", None),
        P("surf", None),
        P(),
    )
    out_specs = (P("probe", "surf"), P("surf"), P("probe"))
    return jax.shard_map(body, mesh=mesh, in_specs=in_specs, out_specs=out_specs, check_vma=False)
```

```python
import functools

import jax
import jax.numpy as jnp
from jax import lax
from jax.experimental import pallas as pl
from jax.experimental.pallas import tpu as pltpu
from jax.sharding import PartitionSpec as P

P_SIZE = 32
BS = 64
PATCH = 128
WIDE = 256
GATHER_BYTES = 4 << 20
F32, BF16 = jnp.float32, jnp.bfloat16
VMEM = pl.BlockSpec(memory_space=pltpu.VMEM)
SMEM = pl.BlockSpec(memory_space=pltpu.SMEM)


def partner(i, shift, size):
    return i ^ shift if size & (size - 1) == 0 else (i + shift) % size


def total_over(part, axis):
    size = lax.axis_size(axis)
    total = part
    for shift in range(size - 1, 0, -1):
        total = total + lax.ppermute(part, axis, [(i, partner(i, shift, size)) for i in range(size)])
    return total


def halving_sum(part, axis):
    size = lax.axis_size(axis)
    if size & (size - 1):
        return lax.psum(part, axis)
    step = 1
    while step < size:
        part = part + lax.ppermute(part, axis, [(i, i ^ step) for i in range(size)])
        step *= 2
    return part


def contract_last(a, b):
    return lax.dot_general(a, b, (((1,), (1,)), ((), ())), preferred_element_type=F32)


def pack_kernel(coef_ref, obs_ref, out_ref):
    slots, vol = coef_ref.shape
    out_ref[:slots, :] = coef_ref[...]
    extra = out_ref.shape[0] - slots
    for t in range(vol // slots):
        out_ref[slots:, t * slots : (t + 1) * slots] = obs_ref[t * extra : (t + 1) * extra, :]


def index_kernel(sigma_ref, owner_ref, perm_ref, counts_ref, pos_ref, pick_ref, sigk_ref):
    blocks = owner_ref.shape[1]
    depth = blocks // lax.axis_size("surf")
    width = pick_ref.shape[0] // blocks
    me = lax.axis_index("surf")
    owner = owner_ref[...]
    wide = jnp.broadcast_to(owner.astype(F32), (blocks, blocks))
    row = lax.broadcasted_iota(jnp.int32, (blocks, blocks), 0)
    lane = lax.broadcasted_iota(jnp.int32, (blocks, blocks), 1)
    same = (wide.T == wide) & (row < lane)
    rank = jnp.sum(jnp.where(same, 1.0, 0.0), axis=0, keepdims=True).astype(jnp.int32)
    pos = (owner ^ me) * depth + rank
    pos_ref[...] = pos
    rows = blocks * width
    at = lax.broadcasted_iota(jnp.int32, (rows, blocks), 0) // width
    perm = jnp.broadcast_to(perm_ref[...].astype(F32), (rows, blocks))
    slot = jnp.sum(jnp.where(jnp.broadcast_to(pos, (rows, blocks)) == at, perm, 0.0), axis=1, keepdims=True)
    slots = lax.broadcasted_iota(jnp.int32, (rows, blocks), 1).astype(F32)
    pick_ref[...] = jnp.where(slots == slot, 1.0, 0.0).astype(BF16)
    patches, patch = sigma_ref.shape
    k = lax.broadcasted_iota(jnp.int32, (patches, blocks), 0)
    b = lax.broadcasted_iota(jnp.int32, (patches, blocks), 1)
    count = jnp.broadcast_to(counts_ref[...].astype(F32), (patches, blocks))
    c = lax.broadcasted_iota(jnp.int32, (patches, patch), 1)
    first = jnp.sum(jnp.where(b == 2 * k, count, 0.0), axis=1, keepdims=True)
    second = jnp.sum(jnp.where(b == 2 * k + 1, count, 0.0), axis=1, keepdims=True)
    column = jnp.where(c < BS, c, c - BS).astype(F32)
    keep = column < jnp.where(c < BS, first, second)
    sigk_ref[...] = jnp.where(keep, sigma_ref[...], 0.0)


def spread_kernel(pos_ref, probes_ref, sigk_ref, patch_ref, sorted_ref, x_ref, m_ref):
    width, nodes = probes_ref.shape
    patch = patch_ref.shape[0]
    for k in range(nodes // patch):
        x_ref[k * width : (k + 1) * width, :] = probes_ref[:, k * patch : (k + 1) * patch].astype(F32)
    m_ref[...] = jnp.dot(x_ref[...].astype(BF16), patch_ref[...], preferred_element_type=F32)
    low = lax.broadcasted_iota(jnp.int32, (width, patch), 1) < BS
    for k in range(nodes // patch):
        s = m_ref[k * width : (k + 1) * width, :] * sigk_ref[k : k + 1, :]
        s = s.astype(BF16).astype(F32)
        r = pltpu.roll(s, BS, 1)
        at0 = pl.multiple_of(pos_ref[0, 2 * k] * width, width)
        at1 = pl.multiple_of(pos_ref[0, 2 * k + 1] * width, width)
        sorted_ref[pl.ds(at0, width), :] = jnp.where(low, s, r)
        sorted_ref[pl.ds(at1, width), :] = jnp.where(low, r, s)


def columns(field, pick, packs, op_ref, coef_ref, obs_ref, lifted_ref, weighted_ref):
    slots = pick.shape[1]
    vol = op_ref.shape[0]
    lanes = field.shape[1]
    each = field.shape[0] // len(packs)
    for r, pack in enumerate(packs):
        rows = slice(r * each, (r + 1) * each)
        chosen = pick[rows, :]
        coef_ref[rows, :] = jnp.dot(chosen, pack[:slots, :], preferred_element_type=F32)
        obs_t = jnp.concatenate(
            [pack[slots:, t * slots : (t + 1) * slots].astype(F32) for t in range(vol // slots)], axis=0
        )
        obs_t = jnp.concatenate([obs_t] * (lanes // BS), axis=0).astype(BF16)
        obs_ref[rows, :] = contract_last(chosen, obs_t)
    for t in range(vol // lanes):
        tile = slice(t * lanes, (t + 1) * lanes)
        lifted_ref[:, tile] = (field * coef_ref[:, tile]).astype(BF16)
    obs = jnp.concatenate([obs_ref[...]] * (WIDE // lanes), axis=1)
    for n in range(vol // WIDE):
        part = slice(n * WIDE, (n + 1) * WIDE)
        state = jnp.dot(lifted_ref[...], op_ref[:, part], preferred_element_type=F32)
        weighted_ref[:, part] = (state * obs).astype(BF16)
    total = jnp.zeros(field.shape, F32)
    for n in range(vol // WIDE):
        part = slice(n * WIDE, (n + 1) * WIDE)
        term = contract_last(weighted_ref[...], op_ref[part, :]) * coef_ref[:, part]
        for h in range(WIDE // lanes):
            total = total + term[:, h * lanes : (h + 1) * lanes]
    return total + pltpu.roll(total, BS, 1)


def near_kernel(n_packs, field_ref, pick_ref, op_ref, *refs):
    packs, (out_ref, *scratch) = refs[:n_packs], refs[n_packs:]
    rows = out_ref.shape[0]
    out_ref[...] = columns(field_ref[:rows, :], pick_ref[:rows, :], packs, op_ref, *scratch)


def last_kernel(
    n_packs, pos_any, near_ref, field_ref, pick_ref, op_ref, probes_ref, sigk_ref, patch_ref, *refs
):
    packs = refs[:n_packs]
    hess_ref, diag_ref, quad_ref, sens_ref, scaled_ref, pos_ref, sem = refs[n_packs : n_packs + 7]
    scratch = refs[n_packs + 7 :]
    copy = pltpu.make_async_copy(pos_any, pos_ref, sem)
    copy.start()
    done = near_ref.shape[0]
    width, nodes = probes_ref.shape
    patch = patch_ref.shape[0]
    sens_ref[:done, :] = near_ref[...]
    sens_ref[done:, :] = columns(field_ref[done:, :], pick_ref[done:, :], packs, op_ref, *scratch)
    copy.wait()
    low = lax.broadcasted_iota(jnp.int32, (width, patch), 1) < BS
    for k in range(nodes // patch):
        at0 = pl.multiple_of(pos_ref[0, 2 * k] * width, width)
        at1 = pl.multiple_of(pos_ref[0, 2 * k + 1] * width, width)
        both = jnp.where(low, sens_ref[pl.ds(at0, width), :], sens_ref[pl.ds(at1, width), :])
        scaled_ref[k * width : (k + 1) * width, :] = both * sigk_ref[k : k + 1, :]
    scaled = scaled_ref[...]
    high = scaled.astype(BF16)
    mid = (scaled - high.astype(F32)).astype(BF16)
    low_part = (scaled - high.astype(F32) - mid.astype(F32)).astype(BF16)
    factor = patch_ref[...]
    back = contract_last(high, factor) + contract_last(mid, factor) + contract_last(low_part, factor)
    quad = jnp.zeros((width, patch), F32)
    for k in range(nodes // patch):
        value = probes_ref[:, k * patch : (k + 1) * patch].astype(F32)
        one = back[k * width : (k + 1) * width, :]
        hess_ref[:, k * patch : (k + 1) * patch] = value + one
        product = value * one
        diag_ref[k : k + 1, :] = jnp.sum(product, axis=0, keepdims=True)
        quad = quad + product
    quad_ref[...] = quad


def params():
    return pltpu.CompilerParams(vmem_limit_bytes=24 << 20)


def cost(flops, moved):
    return pl.CostEstimate(flops=int(flops), bytes_accessed=int(moved), transcendentals=0)


def gather_plan(
    probes, sigma, prior_patch, owner_map, block_perm, col_counts, coef, obs_weight, column_op
):
    width, nodes = probes.shape
    blocks = owner_map.shape[0]
    slots, vol = coef.shape
    peers = lax.axis_size("surf")
    depth = blocks // peers
    rows = blocks * width
    each = depth * width
    patches = nodes // PATCH
    struct = jax.ShapeDtypeStruct

    def to(x, shift):
        return lax.ppermute(x, "surf", [(i, i ^ shift) for i in range(peers)])

    own = pl.pallas_call(
        pack_kernel,
        out_shape=struct((slots + slots * BS // vol, vol), BF16),
        in_specs=[VMEM] * 2,
        out_specs=VMEM,
        compiler_params=params(),
        name="pack",
    )(coef, obs_weight.T)
    held = [None] * peers
    held[0] = own
    for shift in range(2, peers, 2):
        held[shift] = to(own, shift)
    held[1] = to(own, 1)
    for shift in range(2, peers, 2):
        held[shift + 1] = to(held[shift], 1)

    pos, pick, sigk = pl.pallas_call(
        index_kernel,
        out_shape=(struct((1, blocks), jnp.int32), struct((rows, slots), BF16), struct((patches, PATCH), F32)),
        in_specs=[VMEM] * 4,
        out_specs=(VMEM,) * 3,
        compiler_params=params(),
        cost_estimate=cost(2e8, 1e6),
        name="index",
    )(
        sigma.reshape(patches, PATCH),
        owner_map.reshape(1, blocks),
        block_perm.reshape(1, blocks),
        col_counts.reshape(1, blocks),
    )
    field = pl.pallas_call(
        spread_kernel,
        out_shape=struct((rows, PATCH), F32),
        in_specs=[SMEM, VMEM, VMEM, VMEM],
        out_specs=VMEM,
        scratch_shapes=[pltpu.VMEM((rows // 2, PATCH), F32)] * 2,
        compiler_params=params(),
        cost_estimate=cost(2e8, 1e6),
        name="spread",
    )(pos, probes, sigk, prior_patch)

    def scratch(m):
        return [
            pltpu.VMEM((m, vol), F32),
            pltpu.VMEM((m, PATCH), F32),
            pltpu.VMEM((m, vol), BF16),
            pltpu.VMEM((m, vol), BF16),
        ]

    near = max(peers - 2, 2)
    m = near * each
    sens = pl.pallas_call(
        functools.partial(near_kernel, near),
        out_shape=struct((m, PATCH), F32),
        in_specs=[VMEM] * (3 + near),
        out_specs=VMEM,
        scratch_shapes=scratch(m),
        compiler_params=params(),
        cost_estimate=cost(4 * m * vol * vol, 8e6),
        name="near",
    )(field, pick, column_op, *held[:near])
    far = peers - near
    m = far * each
    hess, diag, quad = pl.pallas_call(
        functools.partial(last_kernel, far),
        out_shape=(struct((width, nodes), F32), struct((patches, PATCH), F32), struct((width, PATCH), F32)),
        in_specs=[pl.BlockSpec(memory_space=pl.ANY)] + [VMEM] * (7 + far),
        out_specs=(VMEM,) * 3,
        scratch_shapes=[
            pltpu.VMEM((rows, PATCH), F32),
            pltpu.VMEM((rows // 2, PATCH), F32),
            pltpu.SMEM((1, blocks), jnp.int32),
            pltpu.SemaphoreType.DMA,
        ]
        + scratch(m),
        compiler_params=params(),
        cost_estimate=cost(4 * m * vol * vol, 8e6),
        name="last",
    )(pos, sens, field, pick, column_op, probes, sigk, prior_patch, *held[near:])
    diag_est = (total_over(diag, "probe") / P_SIZE).reshape(nodes)
    return hess, diag_est, halving_sum(jnp.sum(quad, axis=1), "surf")


def column_term(fields, coef_rows, obs_rows, counts, column_op):
    rows, width, cols = fields.shape
    layers = coef_rows.shape[1] // cols
    column = lax.broadcasted_iota(jnp.int32, (rows, cols), 1)
    keep = jnp.where(column < counts[:, None], 1.0, 0.0).astype(F32)
    coef_full = coef_rows.astype(F32).reshape(rows, 1, layers, cols) * keep[:, None, None, :]
    lifted = (fields.astype(F32)[:, :, None, :] * coef_full).astype(BF16)
    state = jnp.dot(lifted.reshape(rows * width, layers * cols), column_op, preferred_element_type=F32)
    weighted = (state.reshape(rows, width, layers, cols) * obs_rows.astype(F32)[:, None, None, :]).astype(BF16)
    adjoint = contract_last(weighted.reshape(rows * width, layers * cols), column_op)
    return jnp.sum(adjoint.reshape(rows, width, layers, cols) * coef_full, axis=2)


def request_plan(
    probes, sigma, prior_patch, owner_map, block_perm, col_counts, coef, obs_weight, column_op
):
    width, nodes = probes.shape
    blocks = owner_map.shape[0]
    peers = lax.axis_size("surf")
    depth = max(1, blocks // peers)
    slots_all = peers * depth
    grouped = probes.reshape(width, nodes // PATCH, PATCH)
    mixed = jnp.einsum("pki,ij->pkj", grouped, prior_patch, preferred_element_type=F32)
    spread = (mixed.reshape(width, nodes) * sigma[None, :]).astype(BF16)
    fields = spread.reshape(width, blocks, BS).transpose(1, 0, 2)
    row_ids = lax.broadcasted_iota(jnp.int32, (blocks, blocks), 0)
    col_ids = lax.broadcasted_iota(jnp.int32, (blocks, blocks), 1)
    same = (owner_map[None, :] == owner_map[:, None]) & (col_ids < row_ids)
    rank = jnp.sum(same.astype(jnp.int32), axis=1)
    position = owner_map * depth + rank
    request = jnp.full((slots_all,), -1, jnp.int32).at[position].set(block_perm).reshape(peers, depth)
    asked = lax.all_to_all(request, "surf", split_axis=0, concat_axis=0, tiled=True)
    wanted = asked >= 0
    safe_asked = jnp.maximum(asked, 0)
    coef_out = jnp.where(wanted[:, :, None], coef[safe_asked], jnp.zeros((), BF16))
    obs_out = jnp.where(wanted[:, :, None], obs_weight[safe_asked], jnp.zeros((), BF16))
    coef_in = lax.all_to_all(coef_out, "surf", split_axis=0, concat_axis=0, tiled=True)
    obs_in = lax.all_to_all(obs_out, "surf", split_axis=0, concat_axis=0, tiled=True)
    coef_rows = coef_in.reshape(slots_all, coef.shape[1])[position]
    obs_rows = obs_in.reshape(slots_all, BS)[position]
    sens = column_term(fields, coef_rows, obs_rows, col_counts, column_op)
    sens = sens.transpose(1, 0, 2).reshape(width, nodes)
    scaled = (sens * sigma[None, :]).reshape(width, nodes // PATCH, PATCH)
    back = jnp.einsum(
        "pkj,ij->pki", scaled, prior_patch.astype(F32), precision=lax.Precision.HIGHEST
    ).reshape(width, nodes)
    values = probes.astype(F32)
    product = values * back
    diag_est = lax.psum(jnp.sum(product, axis=0), "probe") / P_SIZE
    return values + back, diag_est, lax.psum(jnp.sum(product, axis=1), "surf")


def fits_gather(peers, blocks, width, coef):
    return (
        peers >= 4
        and peers & (peers - 1) == 0
        and blocks % peers == 0
        and width == 8
        and coef.shape[0] == blocks == PATCH
        and coef.shape[1] % WIDE == 0
        and peers * coef.size * coef.dtype.itemsize <= GATHER_BYTES
    )


def body(probes, sigma, prior_patch, owner_map, block_perm, col_counts, coef, obs_weight, column_op):
    peers = lax.axis_size("surf")
    small = fits_gather(peers, owner_map.shape[0], probes.shape[0], coef)
    plan = gather_plan if small else request_plan
    return plan(probes, sigma, prior_patch, owner_map, block_perm, col_counts, coef, obs_weight, column_op)


def solution(mesh):
    in_specs = (
        P("probe", "surf"),
        P("surf"),
        P(),
        P("surf"),
        P("surf"),
        P("surf"),
        P("surf", None),
        P("surf", None),
        P(),
    )
    out_specs = (P("probe", "surf"), P("surf"), P("probe"))
    return jax.shard_map(body, mesh=mesh, in_specs=in_specs, out_specs=out_specs, check_vma=False)
```

```python
import functools

import jax
import jax.numpy as jnp
from jax import lax
from jax.experimental import pallas as pl
from jax.experimental.pallas import tpu as pltpu
from jax.sharding import PartitionSpec as P

P_SIZE = 32
BS = 64
PATCH = 128
WIDE = 256
MOST_PEERS = 16
F32, BF16 = jnp.float32, jnp.bfloat16
VMEM = pl.BlockSpec(memory_space=pltpu.VMEM)
SMEM = pl.BlockSpec(memory_space=pltpu.SMEM)
HBM = pl.BlockSpec(memory_space=pltpu.HBM)


def partner(i, shift, size):
    return i ^ shift if size & (size - 1) == 0 else (i + shift) % size


def contract_last(a, b):
    return lax.dot_general(a, b, (((1,), (1,)), ((), ())), preferred_element_type=F32)


def start_kernel(extra, n_through, owner_hbm, perm_hbm, coef_hbm, obs_hbm, *refs):
    through, refs = refs[:n_through], refs[n_through:]
    brought, (own_ref, pos_ref, *asks, owner_ref, perm_ref, sems) = refs[:n_through], refs[n_through:]
    slots, vol = coef_hbm.shape
    blocks = owner_ref.shape[1]
    copies = [
        pltpu.make_async_copy(owner_hbm, owner_ref, sems.at[0]),
        pltpu.make_async_copy(perm_hbm, perm_ref, sems.at[1]),
        pltpu.make_async_copy(coef_hbm, own_ref.at[:slots, :], sems.at[2]),
    ]
    for t in range(vol // slots):
        copies.append(
            pltpu.make_async_copy(
                obs_hbm.at[t * extra : (t + 1) * extra, :],
                own_ref.at[slots:, t * slots : (t + 1) * slots],
                sems.at[3 + t],
            )
        )
    for source, target in zip(through, brought):
        copies.append(pltpu.make_async_copy(source, target, sems.at[len(copies)]))
    for copy in copies:
        copy.start()
    copies[0].wait()
    copies[1].wait()
    peers = lax.axis_size("surf")
    depth = blocks // peers
    me = lax.axis_index("surf")
    owner = owner_ref[...]
    wide = jnp.broadcast_to(owner.astype(F32), (blocks, blocks))
    row = lax.broadcasted_iota(jnp.int32, (blocks, blocks), 0)
    lane = lax.broadcasted_iota(jnp.int32, (blocks, blocks), 1)
    same = (wide.T == wide) & (row < lane)
    rank = jnp.sum(jnp.where(same, 1.0, 0.0), axis=0, keepdims=True).astype(jnp.int32)
    pos = (owner ^ me) * depth + rank
    pos_ref[...] = pos
    perm = jnp.broadcast_to(perm_ref[...].astype(F32), (blocks, blocks))
    here = jnp.broadcast_to(pos, (blocks, blocks)) == row
    slot = jnp.sum(jnp.where(here, perm, 0.0), axis=1, keepdims=True)
    pick = jnp.where(lane.astype(F32) == slot, 1.0, 0.0)
    for g, ask in enumerate(asks):
        n = ask.shape[0]
        ask[...] = pick[g * n : (g + 1) * n, :].astype(BF16)
    for copy in copies[2:]:
        copy.wait()


def spread_kernel(
    pos_ref, probes_ref, sigma_ref, counts_ref, patch_ref, sorted_ref, sigk_ref, x_ref, m_ref
):
    width, _ = probes_ref.shape
    patches, patch = sigma_ref.shape
    blocks = counts_ref.shape[1]
    k = lax.broadcasted_iota(jnp.int32, (patches, blocks), 0)
    b = lax.broadcasted_iota(jnp.int32, (patches, blocks), 1)
    count = jnp.broadcast_to(counts_ref[...].astype(F32), (patches, blocks))
    c = lax.broadcasted_iota(jnp.int32, (patches, patch), 1)
    first = jnp.sum(jnp.where(b == 2 * k, count, 0.0), axis=1, keepdims=True)
    second = jnp.sum(jnp.where(b == 2 * k + 1, count, 0.0), axis=1, keepdims=True)
    column = jnp.where(c < BS, c, c - BS).astype(F32)
    keep = column < jnp.where(c < BS, first, second)
    sigk_ref[...] = jnp.where(keep, sigma_ref[...], 0.0)
    for k in range(patches):
        x_ref[k * width : (k + 1) * width, :] = probes_ref[:, k * patch : (k + 1) * patch].astype(F32)
    m_ref[...] = jnp.dot(x_ref[...].astype(BF16), patch_ref[...], preferred_element_type=F32)
    low = lax.broadcasted_iota(jnp.int32, (width, patch), 1) < BS
    for k in range(patches):
        s = m_ref[k * width : (k + 1) * width, :] * sigk_ref[k : k + 1, :]
        s = s.astype(BF16).astype(F32)
        r = pltpu.roll(s, BS, 1)
        at0 = pl.multiple_of(pos_ref[0, 2 * k] * width, width)
        at1 = pl.multiple_of(pos_ref[0, 2 * k + 1] * width, width)
        sorted_ref[pl.ds(at0, width), :] = jnp.where(low, s, r)
        sorted_ref[pl.ds(at1, width), :] = jnp.where(low, r, s)


def rows_of(packs, asks, vol):
    n = asks[0].shape[0] // len(packs)
    slots = asks[0].shape[1]
    out = [[] for _ in asks]
    for core, pack in enumerate(packs):
        want = jnp.concatenate([ask[core * n : (core + 1) * n, :] for ask in asks], axis=0)
        coef = jnp.dot(want, pack[:slots, :], preferred_element_type=F32)
        obs_t = jnp.concatenate(
            [pack[slots:, t * slots : (t + 1) * slots].astype(F32) for t in range(vol // slots)], axis=0
        )
        obs_t = jnp.concatenate([obs_t] * (PATCH // BS), axis=0).astype(BF16)
        obs = contract_last(want, obs_t)
        for i in range(len(asks)):
            out[i].append((coef[i * n : (i + 1) * n, :].astype(BF16), obs[i * n : (i + 1) * n, :].astype(BF16)))
    return out


def answer_kernel(count, own_ref, other_ref, *refs):
    asks, outs = refs[:count], refs[count:]
    vol = own_ref.shape[1]
    for out, parts in zip(outs, rows_of((own_ref, other_ref), asks, vol)):
        for core, (coef, obs) in enumerate(parts):
            n = coef.shape[0]
            out[core * n : (core + 1) * n, :vol] = coef
            out[core * n : (core + 1) * n, vol:] = obs


def lift_and_weigh(field, rows, op_ref, coef_ref, lifted_ref, weighted_ref):
    m, lanes = field.shape
    vol = op_ref.shape[0]
    count = rows.shape[0]
    width = m // count
    at = lax.broadcasted_iota(jnp.int32, (m, count), 0) // width
    repeat = jnp.where(at == lax.broadcasted_iota(jnp.int32, (m, count), 1), 1.0, 0.0).astype(BF16)
    coef_ref[...] = jnp.dot(repeat, rows[:, :vol], preferred_element_type=F32)
    obs = jnp.dot(repeat, rows[:, vol:], preferred_element_type=F32)
    for t in range(vol // lanes):
        tile = slice(t * lanes, (t + 1) * lanes)
        lifted_ref[:, tile] = (field * coef_ref[:, tile]).astype(BF16)
    obs = jnp.concatenate([obs] * (WIDE // lanes), axis=1)
    quad = jnp.zeros((width, WIDE), F32)
    for n in range(vol // WIDE):
        part = slice(n * WIDE, (n + 1) * WIDE)
        state = jnp.dot(lifted_ref[...], op_ref[:, part], preferred_element_type=F32)
        weighted = state * obs
        weighted_ref[:, part] = weighted.astype(BF16)
        quad = quad + jnp.sum((weighted * state).reshape(count, width, WIDE), axis=0)
    return quad[:, :lanes] + quad[:, lanes:]


def adjoint_sum(weighted_ref, coef_ref, op_ref):
    m, vol = weighted_ref.shape
    total = jnp.zeros((m, PATCH), F32)
    for n in range(vol // WIDE):
        part = slice(n * WIDE, (n + 1) * WIDE)
        term = contract_last(weighted_ref[...], op_ref[part, :]) * coef_ref[:, part]
        for h in range(WIDE // PATCH):
            total = total + term[:, h * PATCH : (h + 1) * PATCH]
    return total + pltpu.roll(total, BS, 1)


def own_kernel(field_ref, ask_ref, own_ref, other_ref, op_ref, sens_ref, quad_ref, coef_ref, lifted_ref, weighted_ref):
    m = sens_ref.shape[0]
    parts = rows_of((own_ref, other_ref), (ask_ref,), own_ref.shape[1])[0]
    rows = jnp.concatenate([jnp.concatenate([coef, obs], axis=1) for coef, obs in parts], axis=0)
    quad_ref[...] = lift_and_weigh(field_ref[:m, :], rows, op_ref, coef_ref, lifted_ref, weighted_ref)
    sens_ref[...] = adjoint_sum(weighted_ref, coef_ref, op_ref)


def weigh_kernel(count, field_ref, own_quad_ref, op_ref, *refs):
    answers = refs[:count]
    weighted_ref, coef_ref, quad_ref, lifted_ref = refs[count:]
    m = weighted_ref.shape[0]
    rows = jnp.concatenate([answer[...] for answer in answers], axis=0)
    field = field_ref[field_ref.shape[0] - m :, :]
    quad = lift_and_weigh(field, rows, op_ref, coef_ref, lifted_ref, weighted_ref)
    quad_ref[...] = quad + own_quad_ref[...]


def back_kernel(
    pos_any,
    own_sens_ref,
    weighted_ref,
    coef_ref,
    op_ref,
    probes_ref,
    sigk_ref,
    patch_ref,
    hess_ref,
    diag_ref,
    sens_ref,
    scaled_ref,
    pos_ref,
    sem,
):
    copy = pltpu.make_async_copy(pos_any, pos_ref, sem)
    copy.start()
    done = own_sens_ref.shape[0]
    width, nodes = probes_ref.shape
    patch = patch_ref.shape[0]
    sens_ref[:done, :] = own_sens_ref[...]
    sens_ref[done:, :] = adjoint_sum(weighted_ref, coef_ref, op_ref)
    copy.wait()
    low = lax.broadcasted_iota(jnp.int32, (width, patch), 1) < BS
    for k in range(nodes // patch):
        at0 = pl.multiple_of(pos_ref[0, 2 * k] * width, width)
        at1 = pl.multiple_of(pos_ref[0, 2 * k + 1] * width, width)
        both = jnp.where(low, sens_ref[pl.ds(at0, width), :], sens_ref[pl.ds(at1, width), :])
        scaled_ref[k * width : (k + 1) * width, :] = both * sigk_ref[k : k + 1, :]
    scaled = scaled_ref[...]
    high = scaled.astype(BF16)
    mid = (scaled - high.astype(F32)).astype(BF16)
    rest = (scaled - high.astype(F32) - mid.astype(F32)).astype(BF16)
    factor = patch_ref[...]
    back = contract_last(high, factor) + contract_last(mid, factor) + contract_last(rest, factor)
    for k in range(nodes // patch):
        value = probes_ref[:, k * patch : (k + 1) * patch].astype(F32)
        one = back[k * width : (k + 1) * width, :]
        hess_ref[:, k * patch : (k + 1) * patch] = value + one
        diag_ref[k : k + 1, :] = jnp.sum(value * one, axis=0, keepdims=True)


def total_kernel(n_diag, *refs):
    diags, quads, (diag_ref, quad_ref) = refs[:n_diag], refs[n_diag:-2], refs[-2:]
    diag = diags[0][...]
    for more in diags[1:]:
        diag = diag + more[...]
    diag_ref[...] = diag / P_SIZE
    quad = quads[0][...]
    for more in quads[1:]:
        quad = quad + more[...]
    quad_ref[...] = jnp.sum(quad.T, axis=0, keepdims=True)


def params():
    return pltpu.CompilerParams(vmem_limit_bytes=24 << 20)


def cost(flops, moved):
    return pl.CostEstimate(flops=int(flops), bytes_accessed=int(moved), transcendentals=0)


def chip_plan(
    probes, sigma, prior_patch, owner_map, block_perm, col_counts, coef, obs_weight, column_op
):
    width, nodes = probes.shape
    blocks = owner_map.shape[0]
    slots, vol = coef.shape
    peers = lax.axis_size("surf")
    depth = blocks // peers
    rows = blocks * width
    patches = nodes // PATCH
    extra = slots * BS // vol
    struct = jax.ShapeDtypeStruct
    shifts = list(range(2, peers, 2))
    order = sorted(shifts, key=lambda s: -bin(s).count("1"))

    def to(x, shift, axis="surf"):
        size = lax.axis_size(axis)
        return lax.ppermute(x, axis, [(i, partner(i, shift, size)) for i in range(size)])

    ask = struct((2 * depth, slots), BF16)
    through = (probes, sigma.reshape(patches, PATCH), col_counts.reshape(1, blocks), prior_patch)
    given = (owner_map.reshape(1, blocks), block_perm.reshape(1, blocks), coef, obs_weight.T) + through
    probes, sigma, counts, prior_patch, own, pos, *asks = pl.pallas_call(
        functools.partial(start_kernel, extra, len(through)),
        out_shape=tuple(struct(x.shape, x.dtype) for x in through)
        + (struct((slots + extra, vol), BF16), struct((1, blocks), jnp.int32))
        + (ask,) * (peers // 2),
        in_specs=[HBM] * len(given),
        out_specs=(VMEM,) * (len(through) + 2 + peers // 2),
        scratch_shapes=[pltpu.VMEM((1, blocks), jnp.int32)] * 2
        + [pltpu.SemaphoreType.DMA((3 + vol // slots + len(through),))],
        compiler_params=params(),
        name="start",
    )(*[pltpu.with_memory_space_constraint(x, pltpu.HBM) for x in given])
    other = to(own, 1)
    asked = {s: to(asks[s // 2], s) for s in order}

    field, sigk = pl.pallas_call(
        spread_kernel,
        out_shape=(struct((rows, PATCH), F32), struct((patches, PATCH), F32)),
        in_specs=[SMEM] + [VMEM] * 4,
        out_specs=(VMEM,) * 2,
        scratch_shapes=[pltpu.VMEM((rows // 2, PATCH), F32)] * 2,
        compiler_params=params(),
        cost_estimate=cost(1e9, 1e6),
        name="spread",
    )(pos, probes, sigma, counts, prior_patch)

    answer = struct((2 * depth, vol + PATCH), BF16)
    answers = pl.pallas_call(
        functools.partial(answer_kernel, len(shifts)),
        out_shape=(answer,) * len(shifts),
        in_specs=[VMEM] * (2 + len(shifts)),
        out_specs=(VMEM,) * len(shifts),
        compiler_params=params(),
        cost_estimate=cost(1e8, 1e6),
        name="answer",
    )(own, other, *[asked[s] for s in shifts])
    got = {s: to(answers[s // 2 - 1], s) for s in order}

    def scratch(m):
        return [pltpu.VMEM((m, vol), F32), pltpu.VMEM((m, vol), BF16), pltpu.VMEM((m, vol), BF16)]

    m = 2 * depth * width
    own_sens, own_quad = pl.pallas_call(
        own_kernel,
        out_shape=(struct((m, PATCH), F32), struct((width, PATCH), F32)),
        in_specs=[VMEM] * 5,
        out_specs=(VMEM,) * 2,
        scratch_shapes=scratch(m),
        compiler_params=params(),
        cost_estimate=cost(4 * m * vol * vol, 4e6),
        name="own",
    )(field, asks[0], own, other, column_op)
    m = rows - m
    weighted, coef_full, quad = pl.pallas_call(
        functools.partial(weigh_kernel, len(shifts)),
        out_shape=(struct((m, vol), BF16), struct((m, vol), F32), struct((width, PATCH), F32)),
        in_specs=[VMEM] * (3 + len(shifts)),
        out_specs=(VMEM,) * 3,
        scratch_shapes=[pltpu.VMEM((m, vol), BF16)],
        compiler_params=params(),
        cost_estimate=cost(2 * m * vol * vol, 4e6),
        name="weigh",
    )(field, own_quad, column_op, *[got[s] for s in shifts])
    bits = [1 << i for i in range(peers.bit_length() - 1)]
    for step in bits[:-1]:
        quad = quad + to(quad, step)
    quads = (quad, to(quad, bits[-1]))

    hess, diag = pl.pallas_call(
        back_kernel,
        out_shape=(struct((width, nodes), F32), struct((patches, PATCH), F32)),
        in_specs=[pl.BlockSpec(memory_space=pl.ANY)] + [VMEM] * 7,
        out_specs=(VMEM,) * 2,
        scratch_shapes=[
            pltpu.VMEM((rows, PATCH), F32),
            pltpu.VMEM((rows // 2, PATCH), F32),
            pltpu.SMEM((1, blocks), jnp.int32),
            pltpu.SemaphoreType.DMA,
        ],
        compiler_params=params(),
        cost_estimate=cost(2 * m * vol * vol, 4e6),
        name="back",
    )(pos, own_sens, weighted, coef_full, column_op, probes, sigk, prior_patch)
    diags = [diag] + [to(diag, s, "probe") for s in range(lax.axis_size("probe") - 1, 0, -1)]
    diag_est, quad = pl.pallas_call(
        functools.partial(total_kernel, len(diags)),
        out_shape=(struct((patches, PATCH), F32), struct((1, width), F32)),
        in_specs=[VMEM] * (len(diags) + len(quads)),
        out_specs=(VMEM,) * 2,
        compiler_params=params(),
        name="total",
    )(*diags, *quads)
    return hess, diag_est.reshape(nodes), quad.reshape(width)


def column_term(fields, coef_rows, obs_rows, counts, column_op):
    rows, width, cols = fields.shape
    layers = coef_rows.shape[1] // cols
    column = lax.broadcasted_iota(jnp.int32, (rows, cols), 1)
    keep = jnp.where(column < counts[:, None], 1.0, 0.0).astype(F32)
    coef_full = coef_rows.astype(F32).reshape(rows, 1, layers, cols) * keep[:, None, None, :]
    lifted = (fields.astype(F32)[:, :, None, :] * coef_full).astype(BF16)
    state = jnp.dot(lifted.reshape(rows * width, layers * cols), column_op, preferred_element_type=F32)
    weighted = (state.reshape(rows, width, layers, cols) * obs_rows.astype(F32)[:, None, None, :]).astype(BF16)
    adjoint = contract_last(weighted.reshape(rows * width, layers * cols), column_op)
    return jnp.sum(adjoint.reshape(rows, width, layers, cols) * coef_full, axis=2)


def request_plan(
    probes, sigma, prior_patch, owner_map, block_perm, col_counts, coef, obs_weight, column_op
):
    width, nodes = probes.shape
    blocks = owner_map.shape[0]
    peers = lax.axis_size("surf")
    depth = max(1, blocks // peers)
    slots_all = peers * depth
    grouped = probes.reshape(width, nodes // PATCH, PATCH)
    mixed = jnp.einsum("pki,ij->pkj", grouped, prior_patch, preferred_element_type=F32)
    spread = (mixed.reshape(width, nodes) * sigma[None, :]).astype(BF16)
    fields = spread.reshape(width, blocks, BS).transpose(1, 0, 2)
    row_ids = lax.broadcasted_iota(jnp.int32, (blocks, blocks), 0)
    col_ids = lax.broadcasted_iota(jnp.int32, (blocks, blocks), 1)
    same = (owner_map[None, :] == owner_map[:, None]) & (col_ids < row_ids)
    rank = jnp.sum(same.astype(jnp.int32), axis=1)
    position = owner_map * depth + rank
    request = jnp.full((slots_all,), -1, jnp.int32).at[position].set(block_perm).reshape(peers, depth)
    asked = lax.all_to_all(request, "surf", split_axis=0, concat_axis=0, tiled=True)
    wanted = asked >= 0
    safe_asked = jnp.maximum(asked, 0)
    coef_out = jnp.where(wanted[:, :, None], coef[safe_asked], jnp.zeros((), BF16))
    obs_out = jnp.where(wanted[:, :, None], obs_weight[safe_asked], jnp.zeros((), BF16))
    coef_in = lax.all_to_all(coef_out, "surf", split_axis=0, concat_axis=0, tiled=True)
    obs_in = lax.all_to_all(obs_out, "surf", split_axis=0, concat_axis=0, tiled=True)
    coef_rows = coef_in.reshape(slots_all, coef.shape[1])[position]
    obs_rows = obs_in.reshape(slots_all, BS)[position]
    sens = column_term(fields, coef_rows, obs_rows, col_counts, column_op)
    sens = sens.transpose(1, 0, 2).reshape(width, nodes)
    scaled = (sens * sigma[None, :]).reshape(width, nodes // PATCH, PATCH)
    back = jnp.einsum(
        "pkj,ij->pki", scaled, prior_patch.astype(F32), precision=lax.Precision.HIGHEST
    ).reshape(width, nodes)
    values = probes.astype(F32)
    product = values * back
    diag_est = lax.psum(jnp.sum(product, axis=0), "probe") / P_SIZE
    return values + back, diag_est, lax.psum(jnp.sum(product, axis=1), "surf")


def asks_directly(peers):
    return 4 <= peers <= MOST_PEERS and peers & (peers - 1) == 0


def body(probes, sigma, prior_patch, owner_map, block_perm, col_counts, coef, obs_weight, column_op):
    plan = chip_plan if asks_directly(lax.axis_size("surf")) else request_plan
    return plan(
        probes, sigma, prior_patch, owner_map, block_perm, col_counts, coef, obs_weight, column_op
    )


def solution(mesh):
    in_specs = (
        P("probe", "surf"),
        P("surf"),
        P(),
        P("surf"),
        P("surf"),
        P("surf"),
        P("surf", None),
        P("surf", None),
        P(),
    )
    out_specs = (P("probe", "surf"), P("surf"), P("probe"))
    return jax.shard_map(body, mesh=mesh, in_specs=in_specs, out_specs=out_specs, check_vma=False)
```
